32 devices in a mesh: dp: 2 (over x), ep_b: 4 (over z), ep_a: 4 (over y, core).
Axes of the slice: x: 2, y: 2, z: 4, core: 2. Of those that a mesh axis runs over, the one named last changes fastest.
Arguments:
- tokens: bfloat16 [32, 1024, 1024], P(('dp', 'ep_b', 'ep_a')), parts along dimension 0
- expert_ids: int32 [32, 1024], P(('dp', 'ep_b', 'ep_a')), parts along dimension 0
- route_order: int32 [32, 1024], P(('dp', 'ep_b', 'ep_a')), parts along dimension 0
- w_route: bfloat16 [1024, 256], replicated
- expert_keys: bfloat16 [16, 256], replicated
- temperature: float32 [], replicated
- w_in: bfloat16 [16, 1024, 4096], P(('ep_b', 'ep_a'))
- b_in: bfloat16 [16, 4096], P(('ep_b', 'ep_a'))
- w_out: bfloat16 [16, 4096, 1024], P(('ep_b', 'ep_a'))
- b_out: bfloat16 [16, 1024], P(('ep_b', 'ep_a'))
Outputs:
- output: bfloat16 [32, 1024, 1024], P(('dp', 'ep_b', 'ep_a')), parts along dimension 0
There are 2 independent parts. The reference program is written for one: setup_inputs(seed, part) draws one part's arguments, and reference() takes and returns one part's arrays. A program takes and returns all parts, laid end to end along the dimension named above; an argument that names none is the same for every part.
All inputs are finite; a program needn't handle non-finite values.
Results may differ from the reference program's by a relative error of at most 0.00349485.
Values are sent between devices in bfloat16 or wider.
A program may use at most 1 GiB of HBM per device.

```python
import jax
import jax.numpy as jnp
from jax import lax

TOKENS_DEV = 1024
MODEL_DIM = 1024
HIDDEN_DIM = 4096
ROUTER_DIM = 256
NUM_EXPERTS = 16
CAPACITY = 80
HOT_SPAN = max(1, NUM_EXPERTS // 4)


def draw_routes(route_key):
    key_list = jax.random.split(route_key, 5)
    shape_ids = (NUM_EXPERTS, TOKENS_DEV)
    spread_ids = jax.random.randint(key_list[0], shape_ids, 0, NUM_EXPERTS)
    hot_pick = jax.random.randint(key_list[1], shape_ids, 0, 4) == 0
    hot_base = jax.random.randint(key_list[2], (NUM_EXPERTS, 1), 0, NUM_EXPERTS)
    hot_ids = (hot_base + jax.random.randint(key_list[3], shape_ids, 0, HOT_SPAN)) % NUM_EXPERTS
    expert_ids = jnp.where(hot_pick, hot_ids, spread_ids).astype(jnp.int32)
    order_keys = jax.random.split(key_list[4], NUM_EXPERTS)
    route_order = jax.vmap(lambda order_key: jax.random.permutation(order_key, TOKENS_DEV))(order_keys)
    return expert_ids, route_order.astype(jnp.int32)


def setup_inputs(seed: int = 0, part: int = 0) -> dict:
    shared_keys = jax.random.split(jax.random.key(seed), 7)
    part_keys = jax.random.split(jax.random.fold_in(jax.random.key(seed + 1), part), 3)
    w_route = jax.random.normal(shared_keys[0], (MODEL_DIM, ROUTER_DIM), jnp.float32) * MODEL_DIM ** -0.5
    expert_keys = jax.random.normal(shared_keys[1], (NUM_EXPERTS, ROUTER_DIM), jnp.float32)
    temperature = jax.random.uniform(shared_keys[2], (), jnp.float32, 0.1, 0.16)
    w_in = jax.random.normal(shared_keys[3], (NUM_EXPERTS, MODEL_DIM, HIDDEN_DIM), jnp.float32) * MODEL_DIM ** -0.5
    b_in = jax.random.normal(shared_keys[4], (NUM_EXPERTS, HIDDEN_DIM), jnp.float32) * 0.5
    w_out = jax.random.normal(shared_keys[5], (NUM_EXPERTS, HIDDEN_DIM, MODEL_DIM), jnp.float32) * HIDDEN_DIM ** -0.5
    b_out = jax.random.normal(shared_keys[6], (NUM_EXPERTS, MODEL_DIM), jnp.float32) * 0.5
    expert_ids, route_order = draw_routes(part_keys[0])
    key_proj = jnp.dot(expert_keys, w_route.T)
    noise_rows = jax.random.normal(part_keys[1], (NUM_EXPERTS, TOKENS_DEV, MODEL_DIM), jnp.float32)
    strength = jax.random.uniform(part_keys[2], (NUM_EXPERTS, TOKENS_DEV, 1), jnp.float32, 0.5, 1.5)
    tokens = noise_rows + strength * key_proj[expert_ids]
    return {
        "tokens": tokens.astype(jnp.bfloat16),
        "expert_ids": expert_ids,
        "route_order": route_order,
        "w_route": w_route.astype(jnp.bfloat16),
        "expert_keys": expert_keys.astype(jnp.bfloat16),
        "temperature": temperature,
        "w_in": w_in.astype(jnp.bfloat16),
        "b_in": b_in.astype(jnp.bfloat16),
        "w_out": w_out.astype(jnp.bfloat16),
        "b_out": b_out.astype(jnp.bfloat16),
    }


def device_route(tok_rows, id_row, order_row, w_route, key_unit, temperature):
    projected = jnp.dot(tok_rows, w_route, preferred_element_type=jnp.float32)
    proj_unit = projected / jnp.sqrt(jnp.sum(projected * projected, axis=1, keepdims=True))
    router_prob = jax.nn.softmax(jnp.dot(proj_unit, key_unit.T) / temperature, axis=1)
    gate_prob = jnp.take_along_axis(router_prob, id_row[:, None], axis=1)[:, 0]
    ranked_ids = id_row[order_row]
    ranked_hot = (ranked_ids[:, None] == jnp.arange(NUM_EXPERTS)[None, :]).astype(jnp.int32)
    ranked_pos = jnp.sum(jnp.cumsum(ranked_hot, axis=0) * ranked_hot, axis=1) - 1
    slot_pos = jnp.zeros((TOKENS_DEV,), jnp.int32).at[order_row].set(ranked_pos)
    dest_slot = jnp.where(slot_pos < CAPACITY, id_row * CAPACITY + slot_pos, NUM_EXPERTS * CAPACITY)
    send_rows = jnp.zeros((NUM_EXPERTS * CAPACITY, MODEL_DIM), jnp.bfloat16).at[dest_slot].set(tok_rows, mode="drop")
    return send_rows, gate_prob, dest_slot


def expert_apply(operands):
    slot_rows, w_first, b_first, w_second, b_second = operands
    hidden = jnp.dot(slot_rows, w_first, preferred_element_type=jnp.float32) + b_first.astype(jnp.float32)
    hidden = jax.nn.gelu(hidden, approximate=False).astype(jnp.bfloat16)
    result = jnp.dot(hidden, w_second, preferred_element_type=jnp.float32) + b_second.astype(jnp.float32)
    return result.astype(jnp.bfloat16)


def reference(tokens, expert_ids, route_order, w_route, expert_keys, temperature, w_in, b_in, w_out, b_out):
    keys_f32 = expert_keys.astype(jnp.float32)
    key_unit = keys_f32 / jnp.sqrt(jnp.sum(keys_f32 * keys_f32, axis=1, keepdims=True))

    def route_one(operands):
        tok_rows, id_row, order_row = operands
        return device_route(tok_rows, id_row, order_row, w_route, key_unit, temperature)

    send_rows, gate_prob, dest_slot = lax.map(route_one, (tokens, expert_ids, route_order))
    grid_rows = send_rows.reshape(NUM_EXPERTS, NUM_EXPERTS, CAPACITY, MODEL_DIM)
    arrived = jnp.swapaxes(grid_rows, 0, 1).reshape(NUM_EXPERTS, NUM_EXPERTS * CAPACITY, MODEL_DIM)
    expert_out = lax.map(expert_apply, (arrived, w_in, b_in, w_out, b_out))
    returned = jnp.swapaxes(expert_out.reshape(NUM_EXPERTS, NUM_EXPERTS, CAPACITY, MODEL_DIM), 0, 1)
    returned = returned.reshape(NUM_EXPERTS, NUM_EXPERTS * CAPACITY, MODEL_DIM)

    def combine_one(operands):
        back_rows, dest_row, gate_row = operands
        picked = jnp.take(back_rows, dest_row, axis=0, mode="fill", fill_value=0)
        return (gate_row[:, None] * picked.astype(jnp.float32)).astype(jnp.bfloat16)

    return lax.map(combine_one, (returned, dest_slot, gate_prob))
```

```python
import functools

import jax
import jax.numpy as jnp
from jax import lax
from jax.experimental import pallas as pl
from jax.experimental.pallas import tpu as pltpu
from jax.sharding import PartitionSpec as P

EXPERT_AXES = ("ep_b", "ep_a")
MESH = pl.DeviceIdType.MESH
F32, BF16, I32 = jnp.float32, jnp.bfloat16, jnp.int32
NT = (((1,), (1,)), ((), ()))


def xor(v, j, bits):
    total = 0
    for k in range(bits):
        total = total + lax.rem(lax.div(v, 1 << k) + lax.div(j, 1 << k), 2) * (1 << k)
    return total


def kernel(dims, tau_ref, ids_ref, order_ref, wr_hbm, keys_ref, b1_ref, b2_ref, tok_hbm, w1_hbm, w2_hbm, out_hbm,
           tok, wr, w1, w2, perm, send, recv, ybuf, back, hbuf, key_b, gate_b, acc, out,
           load_sem, out_sem, d_send, d_recv, r_send, r_recv):
    nb, na, cap = dims
    num_experts = nb * na
    half = num_experts // 2
    tok_dev, width = tok.shape
    hidden = w1.shape[1]
    dp = lax.axis_index("dp")
    my_b, my_a = lax.axis_index("ep_b"), lax.axis_index("ep_a")
    pair = 2 * cap

    def place(j):
        j = jnp.int32(j)
        return xor(my_b, lax.div(j, na), 2), xor(my_a, lax.rem(j, na), 2)

    def expert_of(j):
        b, a = place(j)
        return b * na + a

    def rows_of(slot):
        return pl.ds(pl.multiple_of(slot * cap, 16), cap)

    def exchange(src, dst, send_sem, recv_sem, slot, j):
        b, a = place(j)
        return pltpu.make_async_remote_copy(
            src_ref=src.at[rows_of(slot)], dst_ref=dst.at[rows_of(slot)],
            send_sem=send_sem.at[slot], recv_sem=recv_sem.at[slot],
            device_id=(dp, b, a), device_id_type=MESH)

    loads = [pltpu.make_async_copy(s, d, load_sem.at[k]) for k, (s, d) in enumerate(
        [(tok_hbm.at[0], tok), (wr_hbm, wr), (w1_hbm.at[0], w1), (w2_hbm.at[0], w2)])]
    for c in loads:
        c.start()
    barrier = pltpu.get_barrier_semaphore()

    def greet(j, carry):
        b, a = place(j)
        pl.semaphore_signal(barrier, inc=1, device_id=(dp, b, a), device_id_type=MESH)
        return carry

    lax.fori_loop(1, num_experts, greet, 0)

    ids = ids_ref[...]
    order = order_ref[...]
    hot = (lax.broadcasted_iota(I32, (num_experts, tok_dev), 0) == ids)
    hot_b = jnp.where(hot, 1.0, 0.0).astype(BF16)
    blk = 256
    for t in range(0, tok_dev, blk):
        o = (lax.broadcasted_iota(I32, (blk, tok_dev), 0) + t) == order
        perm[t:t + blk, :] = jnp.where(o, 1.0, 0.0).astype(BF16)
    ranked = jnp.dot(hot_b, perm[...], preferred_element_type=F32)
    tri = jnp.where(lax.broadcasted_iota(I32, (blk, blk), 0) <= lax.broadcasted_iota(I32, (blk, blk), 1), 1.0, 0.0).astype(BF16)
    carry = jnp.zeros((num_experts, 1), F32)
    pos = []
    for t in range(0, tok_dev, blk):
        part = ranked[:, t:t + blk]
        cum = jnp.dot(part.astype(BF16), tri, preferred_element_type=F32) + carry
        carry = cum[:, blk - 1:blk]
        pos.append(jnp.sum(cum * part, axis=0, keepdims=True) - 1.0)
    ranked_pos = jnp.minimum(jnp.concatenate(pos, axis=1), float(cap))
    pos_b = jnp.broadcast_to(ranked_pos, (16, tok_dev)).astype(BF16)
    slot_pos = lax.dot_general(pos_b, perm[...], NT, preferred_element_type=F32)[0:1, :]
    key_row = ids * 128 + slot_pos.astype(I32)

    loads[0].wait()
    row = lax.broadcasted_iota(I32, (pair, tok_dev), 0)

    def permute(i):
        far, near = expert_of(half + i), expert_of(i)
        target = jnp.where(row < cap, far * 128 + row, near * 128 + row - cap)
        one_hot = jnp.where(key_row == target, 1.0, 0.0).astype(BF16)
        return jnp.dot(one_hot, tok[...], preferred_element_type=F32).astype(BF16)

    def pair_rows(i):
        return pl.ds(pl.multiple_of(i * pair, 16), pair)

    first = permute(0)
    send[0:cap, :] = first[0:cap]
    recv[cap:pair, :] = first[cap:]
    send[pair:2 * pair, :] = permute(1)
    pl.semaphore_wait(barrier, num_experts - 1)
    exchange(send, recv, d_send, d_recv, 0, half).start()

    def dispatch(i, c):
        send[pair_rows(i + 1), :] = permute(i + 1)
        exchange(send, recv, d_send, d_recv, 2 * i, half + i).start()
        exchange(send, recv, d_send, d_recv, 2 * i + 1, i).start()
        return c

    lax.fori_loop(1, half - 1, dispatch, 0)

    loads[1].wait()
    keys_f32 = keys_ref[...].astype(F32)
    key_unit = keys_f32 / jnp.sqrt(jnp.sum(keys_f32 * keys_f32, axis=1, keepdims=True))
    tau = tau_ref[0, 0]
    exchange(send, recv, d_send, d_recv, num_experts - 2, num_experts - 1).start()
    exchange(send, recv, d_send, d_recv, num_experts - 1, half - 1).start()
    key_f = key_row.astype(F32)
    for t in range(0, tok_dev, blk):
        r = jnp.dot(tok[t:t + blk, :], wr[...], preferred_element_type=F32)
        unit = r / jnp.sqrt(jnp.sum(r * r, axis=1, keepdims=True))
        logits = lax.dot_general(key_unit, unit, NT, precision=lax.Precision.HIGHEST, preferred_element_type=F32) / tau
        e = jnp.exp(logits - jnp.max(logits, axis=0, keepdims=True))
        prob = e / jnp.sum(e, axis=0, keepdims=True)
        gate = jnp.sum(jnp.where(hot[:, t:t + blk], prob, 0.0), axis=0, keepdims=True)
        for s in range(0, blk, 128):
            gate_b[t + s:t + s + 128, :] = jnp.broadcast_to(gate[:, s:s + 128], (128, 128)).T
            column = jnp.broadcast_to(key_f[:, t + s:t + s + 128], (128, 128)).T
            key_b[t + s:t + s + 128, 0:128] = column
            key_b[t + s:t + s + 128, 128:256] = column

    loads[2].wait()
    loads[3].wait()

    def expert(i):
        x = recv[pair_rows(i), :]

        def first_layer(n, c):
            cols = pl.ds(pl.multiple_of(n * 512, 512), 512)
            h = jnp.dot(x, w1[:, cols], preferred_element_type=F32) + b1_ref[:, cols].astype(F32)
            h = 0.5 * h * (1.0 + lax.erf(h * 0.7071067811865476))
            hbuf[:, cols] = h.astype(BF16)
            return c

        lax.fori_loop(0, hidden // 512, first_layer, 0)

        def second_layer(n, c):
            cols = pl.ds(pl.multiple_of(n * 256, 256), 256)
            y = jnp.dot(hbuf[...], w2[:, cols], preferred_element_type=F32) + b2_ref[:, cols].astype(F32)
            ybuf[pair_rows(i), cols] = y.astype(BF16)
            return c

        lax.fori_loop(0, width // 256, second_layer, 0)

    exchange(send, recv, d_send, d_recv, 0, half).wait_recv()
    expert(0)
    exchange(ybuf, back, r_send, r_recv, 0, half).start()
    back[cap:pair, :] = ybuf[cap:pair, :]

    def process(i, c):
        exchange(send, recv, d_send, d_recv, 2 * i, half + i).wait_recv()
        exchange(send, recv, d_send, d_recv, 2 * i + 1, i).wait_recv()
        expert(i)
        exchange(ybuf, back, r_send, r_recv, 2 * i, half + i).start()
        exchange(ybuf, back, r_send, r_recv, 2 * i + 1, i).start()
        return c

    lax.fori_loop(1, half, process, 0)

    def picked(i, t):
        lane = lax.broadcasted_iota(I32, (1, pair), 1)
        far, near = expert_of(half + i), expert_of(i)
        target = jnp.where(lane < cap, far * 128 + lane, near * 128 + lane - cap).astype(F32)
        one_hot = jnp.where(key_b[t:t + blk, 0:pair] == target, 1.0, 0.0).astype(BF16)
        return jnp.dot(one_hot, back[pair_rows(i), :], preferred_element_type=F32)

    exchange(ybuf, back, r_send, r_recv, 0, half).wait_recv()
    for t in range(0, tok_dev, blk):
        acc[t:t + blk, :] = picked(0, t)

    def combine(i, c):
        exchange(ybuf, back, r_send, r_recv, 2 * i, half + i).wait_recv()
        exchange(ybuf, back, r_send, r_recv, 2 * i + 1, i).wait_recv()
        for t in range(0, tok_dev, blk):
            acc[t:t + blk, :] += picked(i, t)
        return c

    lax.fori_loop(1, half - 1, combine, 0)
    exchange(ybuf, back, r_send, r_recv, num_experts - 2, num_experts - 1).wait_recv()
    exchange(ybuf, back, r_send, r_recv, num_experts - 1, half - 1).wait_recv()
    stores = []
    for k, t in enumerate(range(0, tok_dev, blk)):
        total = acc[t:t + blk, :] + picked(half - 1, t)
        gate = gate_b[t:t + blk, :]
        for w in range(0, width, 128):
            out[t:t + blk, w:w + 128] = (gate * total[:, w:w + 128]).astype(BF16)
        stores.append(pltpu.make_async_copy(out.at[pl.ds(t, blk)], out_hbm.at[0, pl.ds(t, blk)], out_sem.at[k]))
        stores[-1].start()

    def drain(i, c):
        exchange(send, recv, d_send, d_recv, 2 * i, half + i).wait_send()
        exchange(ybuf, back, r_send, r_recv, 2 * i, half + i).wait_send()
        return c

    def drain_near(i, c):
        exchange(send, recv, d_send, d_recv, 2 * i + 1, i).wait_send()
        exchange(ybuf, back, r_send, r_recv, 2 * i + 1, i).wait_send()
        return c

    lax.fori_loop(0, half, drain, 0)
    lax.fori_loop(1, half, drain_near, 0)
    for c in stores:
        c.wait()


def solution(mesh):
    nb, na = mesh.shape["ep_b"], mesh.shape["ep_a"]
    num_experts = nb * na
    tok_spec = P(("dp",) + EXPERT_AXES)
    expert_spec = P(EXPERT_AXES)

    def device_step(tokens, expert_ids, route_order, w_route, expert_keys, value_a11, w_in, b_in, w_out, b_out):
        tok_dev, width = tokens.shape[1], tokens.shape[2]
        hidden = w_in.shape[2]
        cap = (5 * tok_dev + 4 * num_experts - 1) // (4 * num_experts)
        slots = num_experts * cap
        vmem = pl.BlockSpec(memory_space=pltpu.VMEM)
        hbm = pl.BlockSpec(memory_space=pl.ANY)
        smem = pl.BlockSpec(memory_space=pltpu.SMEM)
        dma = pltpu.SemaphoreType.DMA
        return pl.pallas_call(
            functools.partial(kernel, (nb, na, cap)),
            out_shape=jax.ShapeDtypeStruct((1, tok_dev, width), BF16),
            in_specs=[smem, vmem, vmem, hbm, vmem, vmem, vmem, hbm, hbm, hbm],
            out_specs=hbm,
            scratch_shapes=[
                pltpu.VMEM((tok_dev, width), BF16),
                pltpu.VMEM(w_route.shape, BF16),
                pltpu.VMEM((width, hidden), BF16),
                pltpu.VMEM((hidden, width), BF16),
                pltpu.VMEM((tok_dev, tok_dev), BF16),
                pltpu.VMEM((slots, width), BF16),
                pltpu.VMEM((slots, width), BF16),
                pltpu.VMEM((slots, width), BF16),
                pltpu.VMEM((slots, width), BF16),
                pltpu.VMEM((2 * cap, hidden), BF16),
                pltpu.VMEM((tok_dev, 256), F32),
                pltpu.VMEM((tok_dev, 128), F32),
                pltpu.VMEM((tok_dev, width), F32),
                pltpu.VMEM((tok_dev, width), BF16),
                dma((4,)),
                dma((4,)),
                dma((num_experts,)),
                dma((num_experts,)),
                dma((num_experts,)),
                dma((num_experts,)),
            ],
            compiler_params=pltpu.CompilerParams(collective_id=0, has_side_effects=True, vmem_limit_bytes=62 * 2**20),
            name="moe_exchange",
        )(value_a11.reshape(1, 1), expert_ids, route_order, w_route, expert_keys, b_in, b_out, tokens, w_in, w_out)

    return jax.shard_map(
        device_step,
        mesh=mesh,
        in_specs=(tok_spec, tok_spec, tok_spec, P(), P(), P(), expert_spec, expert_spec, expert_spec, expert_spec),
        out_specs=tok_spec,
        check_vma=False,
    )
```

```python
import functools

import jax
import jax.numpy as jnp
from jax import lax
from jax.experimental import pallas as pl
from jax.experimental.pallas import tpu as pltpu
from jax.sharding import PartitionSpec as P

EXPERT_AXES = ("ep_b", "ep_a")
MESH = pl.DeviceIdType.MESH
F32, BF16, I32 = jnp.float32, jnp.bfloat16, jnp.int32
NT = (((1,), (1,)), ((), ()))


def xor(v, j, bits):
    total = 0
    for k in range(bits):
        total = total + lax.rem(lax.div(v, 1 << k) + lax.div(j, 1 << k), 2) * (1 << k)
    return total


def kernel(dims, tau_hbm, ids_hbm, order_hbm, wr_hbm, keys_hbm, b1_hbm, b2_hbm, tok_hbm, w1_hbm, w2_hbm, out,
           tau_ref, ids_ref, order_ref, keys_ref, b1_ref, b2_ref,
           tok, wr, w1, w2, perm, send, recv, ybuf, back, hbuf, key_b, gate_b, acc, last,
           load_sem, d_send, d_recv, r_send, r_recv):
    nb, na, cap = dims
    num_experts = nb * na
    half = num_experts // 2
    tok_dev, width = tok.shape
    hidden = w1.shape[1]
    dp = lax.axis_index("dp")
    my_b, my_a = lax.axis_index("ep_b"), lax.axis_index("ep_a")
    pair = 2 * cap

    def place(j):
        j = jnp.int32(j)
        return xor(my_b, lax.div(j, na), 2), xor(my_a, lax.rem(j, na), 2)

    def expert_of(j):
        b, a = place(j)
        return b * na + a

    def rows_of(slot):
        return pl.ds(pl.multiple_of(slot * cap, 16), cap)

    def exchange(src, dst, send_sem, recv_sem, slot, j):
        b, a = place(j)
        return pltpu.make_async_remote_copy(
            src_ref=src.at[rows_of(slot)], dst_ref=dst.at[rows_of(slot)],
            send_sem=send_sem.at[slot], recv_sem=recv_sem.at[slot],
            device_id=(dp, b, a), device_id_type=MESH)

    barrier = pltpu.get_barrier_semaphore()

    def greet(j, carry):
        b, a = place(j)
        pl.semaphore_signal(barrier, inc=1, device_id=(dp, b, a), device_id_type=MESH)
        return carry

    lax.fori_loop(1, num_experts, greet, 0)
    loads = [pltpu.make_async_copy(s, d, load_sem.at[k]) for k, (s, d) in enumerate([
        (ids_hbm, ids_ref), (order_hbm, order_ref), (tok_hbm.at[0], tok),
        (wr_hbm, wr), (keys_hbm, keys_ref), (tau_hbm, tau_ref), (b1_hbm, b1_ref), (b2_hbm, b2_ref),
        (w1_hbm.at[0], w1), (w2_hbm.at[0], w2)])]
    for c in loads:
        c.start()

    loads[0].wait()
    loads[1].wait()
    ids = ids_ref[...]
    order = order_ref[...]
    hot = (lax.broadcasted_iota(I32, (num_experts, tok_dev), 0) == ids)
    hot_b = jnp.where(hot, 1.0, 0.0).astype(BF16)
    blk = 256
    for t in range(0, tok_dev, blk):
        o = (lax.broadcasted_iota(I32, (blk, tok_dev), 0) + t) == order
        perm[t:t + blk, :] = jnp.where(o, 1.0, 0.0).astype(BF16)
    ranked = jnp.dot(hot_b, perm[...], preferred_element_type=F32)
    tri = jnp.where(lax.broadcasted_iota(I32, (blk, blk), 0) <= lax.broadcasted_iota(I32, (blk, blk), 1), 1.0, 0.0).astype(BF16)
    carry = jnp.zeros((num_experts, 1), F32)
    pos = []
    for t in range(0, tok_dev, blk):
        part = ranked[:, t:t + blk]
        cum = jnp.dot(part.astype(BF16), tri, preferred_element_type=F32) + carry
        carry = cum[:, blk - 1:blk]
        pos.append(jnp.sum(cum * part, axis=0, keepdims=True) - 1.0)
    ranked_pos = jnp.minimum(jnp.concatenate(pos, axis=1), float(cap))
    pos_b = jnp.broadcast_to(ranked_pos, (16, tok_dev)).astype(BF16)
    slot_pos = lax.dot_general(pos_b, perm[...], NT, preferred_element_type=F32)[0:1, :]
    key_row = ids * 128 + slot_pos.astype(I32)

    loads[2].wait()
    row = lax.broadcasted_iota(I32, (pair, tok_dev), 0)

    def permute(i):
        far, near = expert_of(half + i), expert_of(i)
        target = jnp.where(row < cap, far * 128 + row, near * 128 + row - cap)
        one_hot = jnp.where(key_row == target, 1.0, 0.0).astype(BF16)
        return jnp.dot(one_hot, tok[...], preferred_element_type=F32).astype(BF16)

    def pair_rows(i):
        return pl.ds(pl.multiple_of(i * pair, 16), pair)

    first = permute(0)
    send[0:cap, :] = first[0:cap]
    recv[cap:pair, :] = first[cap:]
    send[pair:2 * pair, :] = permute(1)
    pl.semaphore_wait(barrier, num_experts - 1)
    exchange(send, recv, d_send, d_recv, 0, half).start()

    def dispatch(i, c):
        send[pair_rows(i + 1), :] = permute(i + 1)
        exchange(send, recv, d_send, d_recv, 2 * i, half + i).start()
        exchange(send, recv, d_send, d_recv, 2 * i + 1, i).start()
        return c

    lax.fori_loop(1, half - 1, dispatch, 0)

    for c in loads[3:6]:
        c.wait()
    keys_f32 = keys_ref[...].astype(F32)
    key_unit = keys_f32 / jnp.sqrt(jnp.sum(keys_f32 * keys_f32, axis=1, keepdims=True))
    tau = tau_ref[0]
    exchange(send, recv, d_send, d_recv, num_experts - 2, num_experts - 1).start()
    exchange(send, recv, d_send, d_recv, num_experts - 1, half - 1).start()
    key_f = key_row.astype(F32)
    for t in range(0, tok_dev, blk):
        r = jnp.dot(tok[t:t + blk, :], wr[...], preferred_element_type=F32)
        unit = r / jnp.sqrt(jnp.sum(r * r, axis=1, keepdims=True))
        logits = lax.dot_general(key_unit, unit, NT, precision=lax.Precision.HIGHEST, preferred_element_type=F32) / tau
        e = jnp.exp(logits - jnp.max(logits, axis=0, keepdims=True))
        prob = e / jnp.sum(e, axis=0, keepdims=True)
        gate = jnp.sum(jnp.where(hot[:, t:t + blk], prob, 0.0), axis=0, keepdims=True)
        for s in range(0, blk, 128):
            gate_b[t + s:t + s + 128, :] = jnp.broadcast_to(gate[:, s:s + 128], (128, 128)).T
            column = jnp.broadcast_to(key_f[:, t + s:t + s + 128], (128, 128)).T
            key_b[t + s:t + s + 128, 0:128] = column
            key_b[t + s:t + s + 128, 128:256] = column

    for c in loads[6:]:
        c.wait()

    def expert(i):
        x = recv[pair_rows(i), :]

        def first_layer(n, c):
            cols = pl.ds(pl.multiple_of(n * 512, 512), 512)
            h = jnp.dot(x, w1[:, cols], preferred_element_type=F32) + b1_ref[:, cols].astype(F32)
            h = 0.5 * h * (1.0 + lax.erf(h * 0.7071067811865476))
            hbuf[:, cols] = h.astype(BF16)
            return c

        lax.fori_loop(0, hidden // 512, first_layer, 0)

        def second_layer(n, c):
            cols = pl.ds(pl.multiple_of(n * 256, 256), 256)
            y = jnp.dot(hbuf[...], w2[:, cols], preferred_element_type=F32) + b2_ref[:, cols].astype(F32)
            ybuf[pair_rows(i), cols] = y.astype(BF16)
            return c

        lax.fori_loop(0, width // 256, second_layer, 0)

    exchange(send, recv, d_send, d_recv, 0, half).wait_recv()
    expert(0)
    exchange(ybuf, back, r_send, r_recv, 0, half).start()
    back[cap:pair, :] = ybuf[cap:pair, :]

    def process(i, c):
        exchange(send, recv, d_send, d_recv, 2 * i, half + i).wait_recv()
        exchange(send, recv, d_send, d_recv, 2 * i + 1, i).wait_recv()
        expert(i)
        exchange(ybuf, back, r_send, r_recv, 2 * i, half + i).start()
        exchange(ybuf, back, r_send, r_recv, 2 * i + 1, i).start()
        return c

    lax.fori_loop(1, half, process, 0)

    def selector(i, t):
        lane = lax.broadcasted_iota(I32, (1, pair), 1)
        far, near = expert_of(half + i), expert_of(i)
        target = jnp.where(lane < cap, far * 128 + lane, near * 128 + lane - cap).astype(F32)
        return jnp.where(key_b[t:t + blk, 0:pair] == target, 1.0, 0.0).astype(BF16)

    def picked(i, t):
        return jnp.dot(selector(i, t), back[pair_rows(i), :], preferred_element_type=F32)

    exchange(ybuf, back, r_send, r_recv, 0, half).wait_recv()
    for t in range(0, tok_dev, blk):
        acc[t:t + blk, :] = picked(0, t)

    def combine(i, c):
        exchange(ybuf, back, r_send, r_recv, 2 * i, half + i).wait_recv()
        exchange(ybuf, back, r_send, r_recv, 2 * i + 1, i).wait_recv()
        for t in range(0, tok_dev, blk):
            acc[t:t + blk, :] += picked(i, t)
        return c

    lax.fori_loop(1, half - 1, combine, 0)
    for t in range(0, tok_dev, blk):
        last[t:t + blk, :] = selector(half - 1, t)
    exchange(ybuf, back, r_send, r_recv, num_experts - 1, half - 1).wait_recv()
    exchange(ybuf, back, r_send, r_recv, num_experts - 2, num_experts - 1).wait_recv()
    for t in range(0, tok_dev, blk):
        total = acc[t:t + blk, :] + jnp.dot(last[t:t + blk, :], back[pair_rows(half - 1), :], preferred_element_type=F32)
        gate = gate_b[t:t + blk, :]
        for w in range(0, width, 128):
            out[0, t:t + blk, w:w + 128] = (gate * total[:, w:w + 128]).astype(BF16)

    def drain(i, c):
        exchange(send, recv, d_send, d_recv, 2 * i, half + i).wait_send()
        exchange(ybuf, back, r_send, r_recv, 2 * i, half + i).wait_send()
        return c

    def drain_near(i, c):
        exchange(send, recv, d_send, d_recv, 2 * i + 1, i).wait_send()
        exchange(ybuf, back, r_send, r_recv, 2 * i + 1, i).wait_send()
        return c

    lax.fori_loop(0, half, drain, 0)
    lax.fori_loop(1, half, drain_near, 0)


def solution(mesh):
    nb, na = mesh.shape["ep_b"], mesh.shape["ep_a"]
    num_experts = nb * na
    tok_spec = P(("dp",) + EXPERT_AXES)
    expert_spec = P(EXPERT_AXES)

    def device_step(tokens, expert_ids, route_order, w_route, expert_keys, value_a11, w_in, b_in, w_out, b_out):
        tok_dev, width = tokens.shape[1], tokens.shape[2]
        hidden = w_in.shape[2]
        cap = (5 * tok_dev + 4 * num_experts - 1) // (4 * num_experts)
        slots = num_experts * cap
        vmem = pl.BlockSpec(memory_space=pltpu.VMEM)
        hbm = pl.BlockSpec(memory_space=pl.ANY)
        dma = pltpu.SemaphoreType.DMA
        return pl.pallas_call(
            functools.partial(kernel, (nb, na, cap)),
            out_shape=pltpu.VMEM((1, tok_dev, width), BF16),
            in_specs=[hbm] * 10,
            out_specs=vmem,
            scratch_shapes=[
                pltpu.SMEM((1,), F32),
                pltpu.VMEM((1, tok_dev), I32),
                pltpu.VMEM((1, tok_dev), I32),
                pltpu.VMEM(expert_keys.shape, BF16),
                pltpu.VMEM((1, hidden), BF16),
                pltpu.VMEM((1, width), BF16),
                pltpu.VMEM((tok_dev, width), BF16),
                pltpu.VMEM(w_route.shape, BF16),
                pltpu.VMEM((width, hidden), BF16),
                pltpu.VMEM((hidden, width), BF16),
                pltpu.VMEM((tok_dev, tok_dev), BF16),
                pltpu.VMEM((slots, width), BF16),
                pltpu.VMEM((slots, width), BF16),
                pltpu.VMEM((slots, width), BF16),
                pltpu.VMEM((slots, width), BF16),
                pltpu.VMEM((2 * cap, hidden), BF16),
                pltpu.VMEM((tok_dev, 256), F32),
                pltpu.VMEM((tok_dev, 128), F32),
                pltpu.VMEM((tok_dev, width), F32),
                pltpu.VMEM((tok_dev, 2 * cap), BF16),
                dma((10,)),
                dma((num_experts,)),
                dma((num_experts,)),
                dma((num_experts,)),
                dma((num_experts,)),
            ],
            compiler_params=pltpu.CompilerParams(collective_id=0, has_side_effects=True, vmem_limit_bytes=56 * 2**20),
            name="moe_exchange",
        )(value_a11.reshape(1), expert_ids, route_order, w_route, expert_keys, b_in, b_out, tokens, w_in, w_out)

    return jax.shard_map(
        device_step,
        mesh=mesh,
        in_specs=(tok_spec, tok_spec, tok_spec, P(), P(), P(), expert_spec, expert_spec, expert_spec, expert_spec),
        out_specs=tok_spec,
        check_vma=False,
    )
```

```python
import functools

import jax
import jax.numpy as jnp
from jax import lax
from jax.experimental import pallas as pl
from jax.experimental.pallas import tpu as pltpu
from jax.sharding import PartitionSpec as P

EXPERT_AXES = ("ep_b", "ep_a")
MESH = pl.DeviceIdType.MESH
F32, BF16, I32 = jnp.float32, jnp.bfloat16, jnp.int32
NT = (((1,), (1,)), ((), ()))
BLK, LANES = 256, 128


def one(mask, dtype=BF16):
    return jnp.where(mask, 1.0, 0.0).astype(dtype)


def xor(v, j, bits):
    total = 0
    for k in range(bits):
        total = total + lax.rem(lax.div(v, 1 << k) + lax.div(j, 1 << k), 2) * (1 << k)
    return total


def rank_tokens(ids, order, perm, num_experts, cap):
    tok_dev, blk = ids.shape[1], BLK
    hot = lax.broadcasted_iota(I32, (num_experts, tok_dev), 0) == ids
    hot_f = one(hot, F32)
    for t in range(0, tok_dev, blk):
        perm[t:t + blk, :] = one((lax.broadcasted_iota(I32, (blk, tok_dev), 0) + t) == order)
    ranked = jnp.dot(hot_f.astype(BF16), perm[...], preferred_element_type=F32)
    tri = one(lax.broadcasted_iota(I32, (blk, blk), 0) <= lax.broadcasted_iota(I32, (blk, blk), 1))
    count = jnp.zeros((num_experts, 1), F32)
    pos = []
    for t in range(0, tok_dev, blk):
        part = ranked[:, t:t + blk]
        cum = jnp.dot(part.astype(BF16), tri, preferred_element_type=F32) + count
        count = cum[:, blk - 1:]
        pos.append(jnp.sum(cum * part, axis=0, keepdims=True) - 1.0)
    ranked_pos = jnp.minimum(jnp.concatenate(pos, axis=1), float(cap))
    pos_b = jnp.broadcast_to(ranked_pos, (16, tok_dev)).astype(BF16)
    slot = lax.dot_general(pos_b, perm[...], NT, preferred_element_type=F32)[:1, :].astype(I32)
    return hot, hot_f, slot, count


def make_gates(tok, wr, keys_ref, tau, hot, gate_b, columns):
    keys_f32 = keys_ref[...].astype(F32)
    key_unit = keys_f32 / jnp.sqrt(jnp.sum(keys_f32 * keys_f32, axis=1, keepdims=True))
    for t in range(0, tok.shape[0], BLK):
        r = jnp.dot(tok[t:t + BLK, :], wr[...], preferred_element_type=F32)
        unit = r / jnp.sqrt(jnp.sum(r * r, axis=1, keepdims=True))
        logits = lax.dot_general(key_unit, unit, NT, precision=lax.Precision.HIGHEST, preferred_element_type=F32) / tau
        e = jnp.exp(logits - jnp.max(logits, axis=0, keepdims=True))
        prob = e / jnp.sum(e, axis=0, keepdims=True)
        gate = jnp.sum(jnp.where(hot[:, t:t + BLK], prob, 0.0), axis=0, keepdims=True)
        for s in range(0, BLK, LANES):
            rows = slice(t + s, t + s + LANES)
            gate_b[rows, :] = jnp.broadcast_to(gate[:, s:s + LANES], (LANES, LANES)).T
            for ref, row in columns:
                column = jnp.broadcast_to(row[:, rows], (LANES, LANES)).T
                ref[rows, :LANES] = column
                ref[rows, LANES:] = column


def run_expert(weights, src, dst, rows, size):
    w1, w2, b1_ref, b2_ref, hbuf = weights
    x = src[rows, :]

    def first_layer(n, c):
        cols = pl.ds(pl.multiple_of(n * 512, 512), 512)
        h = jnp.dot(x, w1[:, cols], preferred_element_type=F32) + b1_ref[:, cols].astype(F32)
        h = 0.5 * h * (1.0 + lax.erf(h * 0.7071067811865476))
        hbuf[:size, cols] = h.astype(BF16)
        return c

    lax.fori_loop(0, w1.shape[1] // 512, first_layer, 0)

    def second_layer(n, c):
        cols = pl.ds(pl.multiple_of(n * BLK, BLK), BLK)
        y = jnp.dot(hbuf[:size, :], w2[:, cols], preferred_element_type=F32) + b2_ref[:, cols].astype(F32)
        dst[rows, cols] = y.astype(BF16)
        return c

    lax.fori_loop(0, w2.shape[1] // BLK, second_layer, 0)


def full_kernel(dims, tau_hbm, ids_hbm, order_hbm, wr_hbm, keys_hbm, b1_hbm, b2_hbm, tok_hbm, w1_hbm, w2_hbm, out,
           tau_ref, ids_ref, order_ref, keys_ref, b1_ref, b2_ref,
           tok, wr, w1, w2, perm, send, recv, ybuf, back, hbuf, key_b, gate_b, acc, last,
           load_sem, d_send, d_recv, r_send, r_recv):
    nb, na, cap = dims
    num_experts = nb * na
    half = num_experts // 2
    tok_dev, width = tok.shape
    hidden = w1.shape[1]
    dp = lax.axis_index("dp")
    my_b, my_a = lax.axis_index("ep_b"), lax.axis_index("ep_a")
    pair = 2 * cap

    def place(j):
        j = jnp.int32(j)
        return xor(my_b, lax.div(j, na), 2), xor(my_a, lax.rem(j, na), 2)

    def expert_of(j):
        b, a = place(j)
        return b * na + a

    def rows_of(slot):
        return pl.ds(pl.multiple_of(slot * cap, 16), cap)

    def exchange(src, dst, send_sem, recv_sem, slot, j):
        b, a = place(j)
        return pltpu.make_async_remote_copy(
            src_ref=src.at[rows_of(slot)], dst_ref=dst.at[rows_of(slot)],
            send_sem=send_sem.at[slot], recv_sem=recv_sem.at[slot],
            device_id=(dp, b, a), device_id_type=MESH)

    barrier = pltpu.get_barrier_semaphore()

    def greet(j, carry):
        b, a = place(j)
        pl.semaphore_signal(barrier, inc=1, device_id=(dp, b, a), device_id_type=MESH)
        return carry

    lax.fori_loop(1, num_experts, greet, 0)
    loads = [pltpu.make_async_copy(s, d, load_sem.at[k]) for k, (s, d) in enumerate([
        (ids_hbm, ids_ref), (order_hbm, order_ref), (tok_hbm.at[0], tok),
        (wr_hbm, wr), (keys_hbm, keys_ref), (tau_hbm, tau_ref), (b1_hbm, b1_ref), (b2_hbm, b2_ref),
        (w1_hbm.at[0], w1), (w2_hbm.at[0], w2)])]
    for c in loads:
        c.start()

    loads[0].wait()
    loads[1].wait()
    blk = BLK
    hot, _, slot, _ = rank_tokens(ids_ref[...], order_ref[...], perm, num_experts, cap)
    key_row = ids_ref[...] * LANES + slot

    loads[2].wait()
    row = lax.broadcasted_iota(I32, (pair, tok_dev), 0)

    def permute(i):
        far, near = expert_of(half + i), expert_of(i)
        target = jnp.where(row < cap, far * LANES + row, near * LANES + row - cap)
        one_hot = one(key_row == target)
        return jnp.dot(one_hot, tok[...], preferred_element_type=F32).astype(BF16)

    def pair_rows(i):
        return pl.ds(pl.multiple_of(i * pair, 16), pair)

    first = permute(0)
    send[:cap, :] = first[:cap]
    recv[cap:pair, :] = first[cap:]
    send[pair:2 * pair, :] = permute(1)
    pl.semaphore_wait(barrier, num_experts - 1)
    exchange(send, recv, d_send, d_recv, 0, half).start()

    def dispatch(i, c):
        send[pair_rows(i + 1), :] = permute(i + 1)
        exchange(send, recv, d_send, d_recv, 2 * i, half + i).start()
        exchange(send, recv, d_send, d_recv, 2 * i + 1, i).start()
        return c

    lax.fori_loop(1, half - 1, dispatch, 0)

    for c in loads[3:6]:
        c.wait()
    exchange(send, recv, d_send, d_recv, num_experts - 2, num_experts - 1).start()
    exchange(send, recv, d_send, d_recv, num_experts - 1, half - 1).start()
    make_gates(tok, wr, keys_ref, tau_ref[0], hot, gate_b, [(key_b, key_row.astype(F32))])

    for c in loads[6:]:
        c.wait()

    def expert(i):
        run_expert((w1, w2, b1_ref, b2_ref, hbuf), recv, ybuf, pair_rows(i), pair)

    exchange(send, recv, d_send, d_recv, 0, half).wait_recv()
    expert(0)
    exchange(ybuf, back, r_send, r_recv, 0, half).start()
    back[cap:pair, :] = ybuf[cap:pair, :]

    def process(i, c):
        exchange(send, recv, d_send, d_recv, 2 * i, half + i).wait_recv()
        exchange(send, recv, d_send, d_recv, 2 * i + 1, i).wait_recv()
        expert(i)
        exchange(ybuf, back, r_send, r_recv, 2 * i, half + i).start()
        exchange(ybuf, back, r_send, r_recv, 2 * i + 1, i).start()
        return c

    lax.fori_loop(1, half, process, 0)

    def selector(i, t):
        lane = lax.broadcasted_iota(I32, (1, pair), 1)
        far, near = expert_of(half + i), expert_of(i)
        target = jnp.where(lane < cap, far * LANES + lane, near * LANES + lane - cap).astype(F32)
        return one(key_b[t:t + blk, :pair] == target)

    def picked(i, t):
        return jnp.dot(selector(i, t), back[pair_rows(i), :], preferred_element_type=F32)

    exchange(ybuf, back, r_send, r_recv, 0, half).wait_recv()
    for t in range(0, tok_dev, blk):
        acc[t:t + blk, :] = picked(0, t)

    def combine(i, c):
        exchange(ybuf, back, r_send, r_recv, 2 * i, half + i).wait_recv()
        exchange(ybuf, back, r_send, r_recv, 2 * i + 1, i).wait_recv()
        for t in range(0, tok_dev, blk):
            acc[t:t + blk, :] += picked(i, t)
        return c

    lax.fori_loop(1, half - 1, combine, 0)
    for t in range(0, tok_dev, blk):
        last[t:t + blk, :] = selector(half - 1, t)
    exchange(ybuf, back, r_send, r_recv, num_experts - 1, half - 1).wait_recv()
    exchange(ybuf, back, r_send, r_recv, num_experts - 2, num_experts - 1).wait_recv()
    for t in range(0, tok_dev, blk):
        total = acc[t:t + blk, :] + jnp.dot(last[t:t + blk, :], back[pair_rows(half - 1), :], preferred_element_type=F32)
        gate = gate_b[t:t + blk, :]
        for w in range(0, width, LANES):
            out[0, t:t + blk, w:w + LANES] = (gate * total[:, w:w + LANES]).astype(BF16)

    def drain(i, c):
        exchange(send, recv, d_send, d_recv, 2 * i, half + i).wait_send()
        exchange(ybuf, back, r_send, r_recv, 2 * i, half + i).wait_send()
        return c

    def drain_near(i, c):
        exchange(send, recv, d_send, d_recv, 2 * i + 1, i).wait_send()
        exchange(ybuf, back, r_send, r_recv, 2 * i + 1, i).wait_send()
        return c

    lax.fori_loop(0, half, drain, 0)
    lax.fori_loop(1, half, drain_near, 0)


def tight_kernel(dims, tau_hbm, ids_hbm, order_hbm, wr_hbm, keys_hbm, b1_hbm, b2_hbm, tok_hbm, w1_hbm, w2_hbm, out, flag_out,
                 tau_ref, ids_ref, order_ref, keys_ref, b1_ref, b2_ref,
                 tok, wr, w1, w2, perm, s_far, s_near, r_far, r_near, y_far, y_near, b_far, b_near,
                 p_send, p_recv, p_pack, p_back, o_send, o_recv, o_res, o_ret, meta_s, meta_r, flag_s, flag_r,
                 hbuf, key_b, q_b, gate_b, acc, unpack_ref,
                 load_sem, m_sem, p_sem, pb_sem, f_sem, df_send, df_recv, dn_send, dn_recv, do_send, do_recv,
                 rf_send, rf_recv, rn_send, rn_recv, ro_send, ro_recv):
    nb, na, cap, direct, packet = dims
    num_experts = nb * na
    half = num_experts // 2
    over = cap - direct
    steps = half // 2
    tok_dev, width = tok.shape
    hidden = w1.shape[1]
    dp = lax.axis_index("dp")
    my_b, my_a = lax.axis_index("ep_b"), lax.axis_index("ep_a")
    my_half = lax.div(my_b, nb // 2)
    blk = BLK

    def place(j):
        j = jnp.int32(j)
        return xor(my_b, lax.div(j, na), 2), xor(my_a, lax.rem(j, na), 2)

    def expert_of(j):
        b, a = place(j)
        return b * na + a

    def span(start, size):
        return pl.ds(pl.multiple_of(start, 16), size)

    def remote(src, dst, send_sem, recv_sem, j):
        b, a = place(j)
        return pltpu.make_async_remote_copy(src_ref=src, dst_ref=dst, send_sem=send_sem, recv_sem=recv_sem,
                                            device_id=(dp, b, a), device_id_type=MESH)

    def block(src, dst, send_sem, recv_sem, size, i, j):
        rows = span(i * size, size)
        return remote(src.at[rows], dst.at[rows], send_sem.at[i], recv_sem.at[i], j)

    def far_out(i):
        return block(s_far, r_far, df_send, df_recv, direct, i, half + i)

    def near_out(i):
        return block(s_near, r_near, dn_send, dn_recv, cap, i, i)

    def over_out(i):
        return block(o_send, o_recv, do_send, do_recv, over, i, i)

    def far_back(i):
        return block(y_far, b_far, rf_send, rf_recv, direct, i, half + i)

    def near_back(i):
        return block(y_near, b_near, rn_send, rn_recv, cap, i, i)

    def over_back(i):
        return block(o_res, o_ret, ro_send, ro_recv, over, i, i)

    meta_out = remote(meta_s, meta_r, m_sem.at[0], m_sem.at[1], half)
    packet_out = remote(p_send, p_recv, p_sem.at[0], p_sem.at[1], half)
    packet_back = remote(p_pack, p_back, pb_sem.at[0], pb_sem.at[1], half)
    rounds = [remote(flag_s.at[k], flag_r.at[k], f_sem.at[k, 0], f_sem.at[k, 1], j) for k, j in enumerate((4, 2, 1))]
    rounds.append(pltpu.make_async_remote_copy(
        src_ref=flag_s.at[3], dst_ref=flag_r.at[3], send_sem=f_sem.at[3, 0], recv_sem=f_sem.at[3, 1],
        device_id=(1 - dp, my_b, my_a), device_id_type=MESH))

    barrier = pltpu.get_barrier_semaphore()

    def greet(j, carry):
        b, a = place(j)
        pl.semaphore_signal(barrier, inc=1, device_id=(dp, b, a), device_id_type=MESH)
        return carry

    lax.fori_loop(1, num_experts, greet, 0)
    pl.semaphore_signal(barrier, inc=1, device_id=(1 - dp, my_b, my_a), device_id_type=MESH)
    loads = [pltpu.make_async_copy(s, d, load_sem.at[k]) for k, (s, d) in enumerate([
        (ids_hbm, ids_ref), (order_hbm, order_ref), (tok_hbm.at[0], tok),
        (wr_hbm, wr), (keys_hbm, keys_ref), (tau_hbm, tau_ref), (b1_hbm, b1_ref), (b2_hbm, b2_ref),
        (w1_hbm.at[0], w1), (w2_hbm.at[0], w2)])]
    for c in loads:
        c.start()

    loads[0].wait()
    loads[1].wait()
    ids = ids_ref[...]
    hot, hot_f, slot, count = rank_tokens(ids, order_ref[...], perm, num_experts, cap)
    key_row = ids * LANES + slot

    e_col = lax.broadcasted_iota(I32, (num_experts, 1), 0)
    extra = jnp.where(lax.div(e_col, half) != my_half, jnp.clip(count - float(direct), 0.0, float(over)), 0.0)
    extra_b = jnp.broadcast_to(extra, (num_experts, BLK))
    below = jnp.where(lax.broadcasted_iota(I32, (num_experts, num_experts), 1) < lax.broadcasted_iota(I32, (num_experts, num_experts), 0), 1.0, 0.0)
    base_b = jnp.dot(below.astype(BF16), extra_b.astype(BF16), preferred_element_type=F32)
    total_b = base_b[num_experts - 1:, :] + extra_b[num_experts - 1:, :]
    my_flag = jnp.broadcast_to(jnp.where(total_b > float(packet), 1.0, 0.0), (8, BLK))
    meta_s[:num_experts, :] = base_b
    meta_s[num_experts:2 * num_experts, :] = extra_b
    meta_s[2 * num_experts:, :] = my_flag
    base_tok = jnp.sum(hot_f * base_b[:, 0:1], axis=0, keepdims=True).astype(I32)
    is_extra = (lax.div(ids, half) != my_half) & (slot >= direct) & (slot < cap)
    q_row = jnp.where(is_extra, base_tok + slot - direct, -1)

    loads[2].wait()

    def gathered(mask):
        return jnp.dot(one(mask), tok[...], preferred_element_type=F32).astype(BF16)

    def two(first, second, size, axis, other):
        shape = (2 * size, other) if axis == 0 else (other, 2 * size)
        at = lax.broadcasted_iota(I32, shape, axis)
        return jnp.where(at < size, first * LANES + at, second * LANES + at - size)

    def far_keys(b, axis, other):
        return two(expert_of(half + 2 * b), expert_of(half + 2 * b + 1), direct, axis, other)

    def near_keys(b, axis, other):
        return two(expert_of(2 * b), expert_of(2 * b + 1), cap, axis, other)

    p_send[...] = gathered(lax.broadcasted_iota(I32, (packet, tok_dev), 0) == q_row)
    s_far[:2 * direct, :] = gathered(key_row == far_keys(0, 0, tok_dev))
    pl.semaphore_wait(barrier, num_experts)
    meta_out.start()
    packet_out.start()
    first = gathered(key_row == near_keys(0, 0, tok_dev))
    far_out(0).start()
    far_out(1).start()
    r_near[:cap, :] = first[:cap]
    s_near[cap:2 * cap, :] = first[cap:]

    def fill(b, c):
        s_far[span(2 * direct * b, 2 * direct), :] = gathered(key_row == far_keys(b, 0, tok_dev))
        s_near[span(2 * cap * b, 2 * cap), :] = gathered(key_row == near_keys(b, 0, tok_dev))
        return c

    lax.fori_loop(1, steps, fill, 0)

    for c in loads[3:6]:
        c.wait()
    make_gates(tok, wr, keys_ref, tau_ref[0], hot, gate_b, [(key_b, key_row.astype(F32)), (q_b, q_row.astype(F32))])

    meta_out.wait_recv()
    packet_out.wait_recv()
    q_lane = lax.broadcasted_iota(I32, (over, packet), 1).astype(F32)
    r_sub = lax.broadcasted_iota(I32, (over, packet), 0).astype(F32)
    picks = []
    lane = lax.broadcasted_iota(I32, (1, half * over), 1)
    home = jnp.full((1, half * over), -1.0, F32)
    for j in range(half):
        e = expert_of(j)
        base = meta_r[pl.ds(e, 1), :]
        size = meta_r[pl.ds(num_experts + e, 1), :]
        picks.append(one((q_lane - r_sub) == base[:, :packet]))
        at = (lane - j * over).astype(F32)
        home = jnp.where((at >= 0.0) & (at < size), base + at, home)
    forward = jnp.dot(jnp.concatenate(picks, axis=0), p_recv[...], preferred_element_type=F32).astype(BF16)
    o_recv[:over, :] = forward[:over]
    o_send[over:, :] = forward[over:]
    known = jnp.maximum(my_flag, meta_r[2 * num_experts:, :])
    flag_s[0] = known
    unpack = one(lax.broadcasted_iota(I32, (packet, half * over), 0).astype(F32) == home)

    def start_all(make):
        def go(i, c):
            make(i).start()
            return c
        lax.fori_loop(1, half, go, 0)

    start_all(over_out)
    rounds[0].start()
    near_out(1).start()

    def dispatch(b, c):
        for make, i in ((far_out, 2 * b), (near_out, 2 * b), (far_out, 2 * b + 1), (near_out, 2 * b + 1)):
            make(i).start()
        return c

    lax.fori_loop(1, steps, dispatch, 0)
    for c in loads[6:]:
        c.wait()

    def expert(src, dst, start, size):
        run_expert((w1, w2, b1_ref, b2_ref, hbuf), src, dst, span(start, size), size)

    def next_round(k):
        rounds[k].wait_recv()
        if k + 1 < len(rounds):
            flag_s[k + 1] = jnp.maximum(flag_s[k], flag_r[k])

    def step(b, c):
        far_out(2 * b).wait_recv()
        far_out(2 * b + 1).wait_recv()
        expert(r_far, y_far, 2 * direct * b, 2 * direct)
        far_back(2 * b).start()
        far_back(2 * b + 1).start()

        @pl.when(b > 0)
        def _():
            near_out(2 * b).wait_recv()

        near_out(2 * b + 1).wait_recv()
        expert(r_near, y_near, 2 * cap * b, 2 * cap)

        @pl.when(b > 0)
        def _():
            near_back(2 * b).start()

        near_back(2 * b + 1).start()

        @pl.when(b == 0)
        def _():
            def arrived(i, c):
                over_out(i).wait_recv()
                return c

            lax.fori_loop(1, half, arrived, 0)
            expert(o_recv, o_res, 0, half * over)
            o_ret[:over, :] = o_res[:over, :]
            start_all(over_back)

        @pl.when(b == 1)
        def _():
            next_round(0)
            rounds[1].start()

        return c

    unpack_ref[...] = unpack
    lax.fori_loop(0, steps, step, 0)
    b_near[:cap, :] = y_near[:cap, :]
    next_round(1)

    def returned(i, c):
        over_back(i).wait_recv()
        return c

    lax.fori_loop(1, half, returned, 0)
    p_pack[...] = jnp.dot(unpack_ref[...], o_ret[...], preferred_element_type=F32).astype(BF16)
    rounds[2].start()
    packet_back.start()

    def add(ref, start, keys, src, fresh=False):
        size = keys.shape[1]
        for t in range(0, tok_dev, blk):
            one_hot = one(ref[t:t + blk, :size] == keys)
            part = jnp.dot(one_hot, src[span(start, size), :], preferred_element_type=F32)
            acc[t:t + blk, :] = part if fresh else acc[t:t + blk, :] + part

    far_back(0).wait_recv()
    far_back(1).wait_recv()
    add(key_b, 0, far_keys(0, 1, 1).astype(F32), b_far, fresh=True)
    next_round(2)

    def near_sum(b, c):
        @pl.when(b > 0)
        def _():
            near_back(2 * b).wait_recv()
        near_back(2 * b + 1).wait_recv()
        add(key_b, 2 * cap * b, near_keys(b, 1, 1).astype(F32), b_near)
        return c

    lax.fori_loop(0, steps, near_sum, 0)
    rounds[3].start()

    def far_sum(b, c):
        far_back(2 * b).wait_recv()
        far_back(2 * b + 1).wait_recv()
        add(key_b, 2 * direct * b, far_keys(b, 1, 1).astype(F32), b_far)
        return c

    far_sum(1, 0)
    packet_back.wait_recv()
    add(q_b, 0, lax.broadcasted_iota(I32, (1, packet), 1).astype(F32), p_back)
    next_round(3)
    flag_s[4] = jnp.maximum(flag_s[3], flag_r[3])
    far_sum(2, 0)
    flag_out[0] = flag_s[4][0, 0].astype(I32)
    far_back(half - 2).wait_recv()
    far_back(half - 1).wait_recv()
    keys = far_keys(steps - 1, 1, 1).astype(F32)
    for t in range(0, tok_dev, blk):
        one_hot = one(key_b[t:t + blk, 0:2 * direct] == keys)
        total = acc[t:t + blk, :] + jnp.dot(one_hot, b_far[direct * (half - 2):, :], preferred_element_type=F32)
        gate = gate_b[t:t + blk, :]
        for w in range(0, width, LANES):
            out[0, t:t + blk, w:w + LANES] = (gate * total[:, w:w + LANES]).astype(BF16)

    def drain_far(i, c):
        far_out(i).wait_send()
        far_back(i).wait_send()
        return c

    def drain(i, c):
        near_out(i).wait_send()
        near_back(i).wait_send()
        over_out(i).wait_send()
        over_back(i).wait_send()
        return c

    lax.fori_loop(0, half, drain_far, 0)
    lax.fori_loop(1, half, drain, 0)
    for c in [meta_out, packet_out, packet_back] + rounds:
        c.wait_send()


def solution(mesh):
    nb, na = mesh.shape["ep_b"], mesh.shape["ep_a"]
    num_experts = nb * na
    half = num_experts // 2
    tok_spec = P(("dp",) + EXPERT_AXES)
    expert_spec = P(EXPERT_AXES)

    def device_step(tokens, expert_ids, route_order, w_route, expert_keys, value_a11, w_in, b_in, w_out, b_out):
        tok_dev, width = tokens.shape[1], tokens.shape[2]
        hidden = w_in.shape[2]
        cap = (5 * tok_dev + 4 * num_experts - 1) // (4 * num_experts)
        direct = 3 * tok_dev // (4 * num_experts)
        over = cap - direct
        packet = 11 * tok_dev // 64
        slots = num_experts * cap
        vmem = pl.BlockSpec(memory_space=pltpu.VMEM)
        hbm = pl.BlockSpec(memory_space=pl.ANY)
        dma = pltpu.SemaphoreType.DMA

        def rows(n, dtype=BF16, lanes=width):
            return pltpu.VMEM((n, lanes), dtype)

        operands = [
            pltpu.SMEM((1,), F32),
            rows(1, I32, tok_dev),
            rows(1, I32, tok_dev),
            rows(num_experts, BF16, expert_keys.shape[1]),
            rows(1, BF16, hidden),
            rows(1),
            rows(tok_dev),
            rows(width, BF16, w_route.shape[1]),
            rows(width, BF16, hidden),
            rows(hidden),
            rows(tok_dev, BF16, tok_dev),
        ]
        args = (value_a11.reshape(1), expert_ids, route_order, w_route, expert_keys, b_in, b_out, tokens, w_in, w_out)
        result = pltpu.VMEM((1, tok_dev, width), BF16)

        def full(*args):
            return pl.pallas_call(
                functools.partial(full_kernel, (nb, na, cap)),
                out_shape=result,
                in_specs=[hbm] * 10,
                out_specs=vmem,
                scratch_shapes=operands + [
                    rows(slots), rows(slots), rows(slots), rows(slots),
                    rows(2 * cap, BF16, hidden),
                    rows(tok_dev, F32, 256),
                    rows(tok_dev, F32, 128),
                    rows(tok_dev, F32),
                    rows(tok_dev, BF16, 2 * cap),
                    dma((10,)),
                ] + [dma((num_experts,))] * 4,
                compiler_params=pltpu.CompilerParams(collective_id=1, has_side_effects=True, vmem_limit_bytes=56 * 2**20),
                name="full_exchange",
            )(*args)

        far, near, extra = half * direct, half * cap, half * over
        out, flag = pl.pallas_call(
            functools.partial(tight_kernel, (nb, na, cap, direct, packet)),
            out_shape=(result, pltpu.SMEM((1,), I32)),
            in_specs=[hbm] * 10,
            out_specs=(vmem, pl.BlockSpec(memory_space=pltpu.SMEM)),
            scratch_shapes=operands + [
                rows(far), rows(near), rows(far), rows(near), rows(far), rows(near), rows(far), rows(near),
                rows(packet), rows(packet), rows(packet), rows(packet),
                rows(extra), rows(extra), rows(extra), rows(extra),
                rows(40, F32, 256), rows(40, F32, 256),
                pltpu.VMEM((5, 8, 256), F32), pltpu.VMEM((4, 8, 256), F32),
                rows(max(extra, 2 * cap), BF16, hidden),
                rows(tok_dev, F32, 256),
                rows(tok_dev, F32, 256),
                rows(tok_dev, F32, 128),
                rows(tok_dev, F32),
                rows(packet, BF16, extra),
                dma((10,)), dma((2,)), dma((2,)), dma((2,)), dma((4, 2)),
            ] + [dma((half,))] * 12,
            compiler_params=pltpu.CompilerParams(collective_id=0, has_side_effects=True, vmem_limit_bytes=61 * 2**20),
            name="tight_exchange",
        )(*args)
        return lax.cond(flag[0] > 0, lambda out, *args: full(*args), lambda out, *args: out, out, *args)

    return jax.shard_map(
        device_step,
        mesh=mesh,
        in_specs=(tok_spec, tok_spec, tok_spec, P(), P(), P(), expert_spec, expert_spec, expert_spec, expert_spec),
        out_specs=tok_spec,
        check_vma=False,
    )
```

```python
import functools

import jax
import jax.numpy as jnp
from jax import lax
from jax.experimental import pallas as pl
from jax.experimental.pallas import tpu as pltpu
from jax.sharding import PartitionSpec as P

EXPERT_AXES = ("ep_b", "ep_a")
MESH = pl.DeviceIdType.MESH
F32, BF16, I32 = jnp.float32, jnp.bfloat16, jnp.int32
NT = (((1,), (1,)), ((), ()))
BLK, LANES = 256, 128


def one(mask, dtype=BF16):
    return jnp.where(mask, 1.0, 0.0).astype(dtype)


def xor(v, j, bits):
    total = 0
    for k in range(bits):
        total = total + lax.rem(lax.div(v, 1 << k) + lax.div(j, 1 << k), 2) * (1 << k)
    return total


def rank_tokens(ids, order, perm, num_experts, cap):
    tok_dev, blk = ids.shape[1], BLK
    hot = lax.broadcasted_iota(I32, (num_experts, tok_dev), 0) == ids
    hot_f = one(hot, F32)
    for t in range(0, tok_dev, blk):
        perm[t:t + blk, :] = one((lax.broadcasted_iota(I32, (blk, tok_dev), 0) + t) == order)
    ranked = jnp.dot(hot_f.astype(BF16), perm[...], preferred_element_type=F32)
    tri = one(lax.broadcasted_iota(I32, (blk, blk), 0) <= lax.broadcasted_iota(I32, (blk, blk), 1))
    count = jnp.zeros((num_experts, 1), F32)
    pos = []
    for t in range(0, tok_dev, blk):
        part = ranked[:, t:t + blk]
        cum = jnp.dot(part.astype(BF16), tri, preferred_element_type=F32) + count
        count = cum[:, blk - 1:]
        pos.append(jnp.sum(cum * part, axis=0, keepdims=True) - 1.0)
    ranked_pos = jnp.minimum(jnp.concatenate(pos, axis=1), float(cap))
    pos_b = jnp.broadcast_to(ranked_pos, (16, tok_dev)).astype(BF16)
    slot = lax.dot_general(pos_b, perm[...], NT, preferred_element_type=F32)[:1, :].astype(I32)
    return hot, hot_f, slot, count


def make_gates(tok, wr, keys_ref, tau, hot, gate_b, columns):
    keys_f32 = keys_ref[...].astype(F32)
    key_unit = keys_f32 / jnp.sqrt(jnp.sum(keys_f32 * keys_f32, axis=1, keepdims=True))
    for t in range(0, tok.shape[0], BLK):
        r = jnp.dot(tok[t:t + BLK, :], wr[...], preferred_element_type=F32)
        unit = r / jnp.sqrt(jnp.sum(r * r, axis=1, keepdims=True))
        logits = lax.dot_general(key_unit, unit, NT, precision=lax.Precision.HIGHEST, preferred_element_type=F32) / tau
        e = jnp.exp(logits - jnp.max(logits, axis=0, keepdims=True))
        prob = e / jnp.sum(e, axis=0, keepdims=True)
        gate = jnp.sum(jnp.where(hot[:, t:t + BLK], prob, 0.0), axis=0, keepdims=True)
        for s in range(0, BLK, LANES):
            rows = slice(t + s, t + s + LANES)
            gate_b[rows, :] = jnp.broadcast_to(gate[:, s:s + LANES], (LANES, LANES)).T
            for ref, row in columns:
                column = jnp.broadcast_to(row[:, rows], (LANES, LANES)).T
                ref[rows, :LANES] = column
                ref[rows, LANES:] = column


def run_expert(weights, src, dst, rows, size):
    w1, w2, b1_ref, b2_ref, hbuf = weights
    x = src[rows, :]

    def first_layer(n, c):
        cols = pl.ds(pl.multiple_of(n * 512, 512), 512)
        h = jnp.dot(x, w1[:, cols], preferred_element_type=F32) + b1_ref[:, cols].astype(F32)
        h = 0.5 * h * (1.0 + lax.erf(h * 0.7071067811865476))
        hbuf[:size, cols] = h.astype(BF16)
        return c

    lax.fori_loop(0, w1.shape[1] // 512, first_layer, 0)

    def second_layer(n, c):
        cols = pl.ds(pl.multiple_of(n * BLK, BLK), BLK)
        y = jnp.dot(hbuf[:size, :], w2[:, cols], preferred_element_type=F32) + b2_ref[:, cols].astype(F32)
        dst[rows, cols] = y.astype(BF16)
        return c

    lax.fori_loop(0, w2.shape[1] // BLK, second_layer, 0)


def full_kernel(dims, tau_hbm, ids_hbm, order_hbm, wr_hbm, keys_hbm, b1_hbm, b2_hbm, tok_hbm, w1_hbm, w2_hbm, out,
           tau_ref, ids_ref, order_ref, keys_ref, b1_ref, b2_ref,
           tok, wr, w1, w2, perm, send, recv, ybuf, back, hbuf, key_b, gate_b, acc, last,
           load_sem, d_send, d_recv, r_send, r_recv):
    nb, na, cap = dims
    num_experts = nb * na
    half = num_experts // 2
    tok_dev, width = tok.shape
    hidden = w1.shape[1]
    dp = lax.axis_index("dp")
    my_b, my_a = lax.axis_index("ep_b"), lax.axis_index("ep_a")
    pair = 2 * cap

    def place(j):
        j = jnp.int32(j)
        return xor(my_b, lax.div(j, na), 2), xor(my_a, lax.rem(j, na), 2)

    def expert_of(j):
        b, a = place(j)
        return b * na + a

    def rows_of(slot):
        return pl.ds(pl.multiple_of(slot * cap, 16), cap)

    def exchange(src, dst, send_sem, recv_sem, slot, j):
        b, a = place(j)
        return pltpu.make_async_remote_copy(
            src_ref=src.at[rows_of(slot)], dst_ref=dst.at[rows_of(slot)],
            send_sem=send_sem.at[slot], recv_sem=recv_sem.at[slot],
            device_id=(dp, b, a), device_id_type=MESH)

    barrier = pltpu.get_barrier_semaphore()

    def greet(j, carry):
        b, a = place(j)
        pl.semaphore_signal(barrier, inc=1, device_id=(dp, b, a), device_id_type=MESH)
        return carry

    lax.fori_loop(1, num_experts, greet, 0)
    loads = [pltpu.make_async_copy(s, d, load_sem.at[k]) for k, (s, d) in enumerate([
        (ids_hbm, ids_ref), (order_hbm, order_ref), (tok_hbm.at[0], tok),
        (wr_hbm, wr), (keys_hbm, keys_ref), (tau_hbm, tau_ref), (b1_hbm, b1_ref), (b2_hbm, b2_ref),
        (w1_hbm.at[0], w1), (w2_hbm.at[0], w2)])]
    for c in loads:
        c.start()

    loads[0].wait()
    loads[1].wait()
    blk = BLK
    hot, _, slot, _ = rank_tokens(ids_ref[...], order_ref[...], perm, num_experts, cap)
    key_row = ids_ref[...] * LANES + slot

    loads[2].wait()
    row = lax.broadcasted_iota(I32, (pair, tok_dev), 0)

    def permute(i):
        far, near = expert_of(half + i), expert_of(i)
        target = jnp.where(row < cap, far * LANES + row, near * LANES + row - cap)
        one_hot = one(key_row == target)
        return jnp.dot(one_hot, tok[...], preferred_element_type=F32).astype(BF16)

    def pair_rows(i):
        return pl.ds(pl.multiple_of(i * pair, 16), pair)

    first = permute(0)
    send[:cap, :] = first[:cap]
    recv[cap:pair, :] = first[cap:]
    send[pair:2 * pair, :] = permute(1)
    pl.semaphore_wait(barrier, num_experts - 1)
    exchange(send, recv, d_send, d_recv, 0, half).start()

    def dispatch(i, c):
        send[pair_rows(i + 1), :] = permute(i + 1)
        exchange(send, recv, d_send, d_recv, 2 * i, half + i).start()
        exchange(send, recv, d_send, d_recv, 2 * i + 1, i).start()
        return c

    lax.fori_loop(1, half - 1, dispatch, 0)

    for c in loads[3:6]:
        c.wait()
    exchange(send, recv, d_send, d_recv, num_experts - 2, num_experts - 1).start()
    exchange(send, recv, d_send, d_recv, num_experts - 1, half - 1).start()
    make_gates(tok, wr, keys_ref, tau_ref[0], hot, gate_b, [(key_b, key_row.astype(F32))])

    for c in loads[6:]:
        c.wait()

    def expert(i):
        run_expert((w1, w2, b1_ref, b2_ref, hbuf), recv, ybuf, pair_rows(i), pair)

    exchange(send, recv, d_send, d_recv, 0, half).wait_recv()
    expert(0)
    exchange(ybuf, back, r_send, r_recv, 0, half).start()
    back[cap:pair, :] = ybuf[cap:pair, :]

    def process(i, c):
        exchange(send, recv, d_send, d_recv, 2 * i, half + i).wait_recv()
        exchange(send, recv, d_send, d_recv, 2 * i + 1, i).wait_recv()
        expert(i)
        exchange(ybuf, back, r_send, r_recv, 2 * i, half + i).start()
        exchange(ybuf, back, r_send, r_recv, 2 * i + 1, i).start()
        return c

    lax.fori_loop(1, half, process, 0)

    def selector(i, t):
        lane = lax.broadcasted_iota(I32, (1, pair), 1)
        far, near = expert_of(half + i), expert_of(i)
        target = jnp.where(lane < cap, far * LANES + lane, near * LANES + lane - cap).astype(F32)
        return one(key_b[t:t + blk, :pair] == target)

    def picked(i, t):
        return jnp.dot(selector(i, t), back[pair_rows(i), :], preferred_element_type=F32)

    exchange(ybuf, back, r_send, r_recv, 0, half).wait_recv()
    for t in range(0, tok_dev, blk):
        acc[t:t + blk, :] = picked(0, t)

    def combine(i, c):
        exchange(ybuf, back, r_send, r_recv, 2 * i, half + i).wait_recv()
        exchange(ybuf, back, r_send, r_recv, 2 * i + 1, i).wait_recv()
        for t in range(0, tok_dev, blk):
            acc[t:t + blk, :] += picked(i, t)
        return c

    lax.fori_loop(1, half - 1, combine, 0)
    for t in range(0, tok_dev, blk):
        last[t:t + blk, :] = selector(half - 1, t)
    exchange(ybuf, back, r_send, r_recv, num_experts - 1, half - 1).wait_recv()
    exchange(ybuf, back, r_send, r_recv, num_experts - 2, num_experts - 1).wait_recv()
    for t in range(0, tok_dev, blk):
        total = acc[t:t + blk, :] + jnp.dot(last[t:t + blk, :], back[pair_rows(half - 1), :], preferred_element_type=F32)
        gate = gate_b[t:t + blk, :]
        for w in range(0, width, LANES):
            out[0, t:t + blk, w:w + LANES] = (gate * total[:, w:w + LANES]).astype(BF16)

    def drain(i, c):
        exchange(send, recv, d_send, d_recv, 2 * i, half + i).wait_send()
        exchange(ybuf, back, r_send, r_recv, 2 * i, half + i).wait_send()
        return c

    def drain_near(i, c):
        exchange(send, recv, d_send, d_recv, 2 * i + 1, i).wait_send()
        exchange(ybuf, back, r_send, r_recv, 2 * i + 1, i).wait_send()
        return c

    lax.fori_loop(0, half, drain, 0)
    lax.fori_loop(1, half, drain_near, 0)


def tight_kernel(dims, tau_hbm, ids_hbm, order_hbm, wr_hbm, keys_hbm, b1_hbm, b2_hbm, tok_hbm, w1_hbm, w2_hbm, out, flag_out,
                 tau_ref, ids_ref, order_ref, keys_ref, b1_ref, b2_ref,
                 tok, wr, w1, w2, perm, s_far, s_near, r_far, r_near, y_far, y_near, b_far, b_near,
                 p_send, p_recv, p_pack, p_back, o_send, o_recv, o_res, o_ret, meta_s, meta_r, flag_s, flag_r,
                 hbuf, key_b, q_b, gate_b, acc, unpack_ref,
                 load_sem, m_sem, p_sem, pb_sem, f_sem, df_send, df_recv, dn_send, dn_recv, do_send, do_recv,
                 rf_send, rf_recv, rn_send, rn_recv, ro_send, ro_recv):
    nb, na, cap, direct, packet = dims
    num_experts = nb * na
    half = num_experts // 2
    over = cap - direct
    steps = half // 2
    early = 1
    tok_dev, width = tok.shape
    hidden = w1.shape[1]
    dp = lax.axis_index("dp")
    my_b, my_a = lax.axis_index("ep_b"), lax.axis_index("ep_a")
    my_half = lax.div(my_b, nb // 2)
    blk = BLK

    def place(j):
        j = jnp.int32(j)
        return xor(my_b, lax.div(j, na), 2), xor(my_a, lax.rem(j, na), 2)

    def expert_of(j):
        b, a = place(j)
        return b * na + a

    def span(start, size):
        return pl.ds(pl.multiple_of(start, 16), size)

    def remote(src, dst, send_sem, recv_sem, j):
        b, a = place(j)
        return pltpu.make_async_remote_copy(src_ref=src, dst_ref=dst, send_sem=send_sem, recv_sem=recv_sem,
                                            device_id=(dp, b, a), device_id_type=MESH)

    def block(src, dst, send_sem, recv_sem, size, i, j):
        rows = span(i * size, size)
        return remote(src.at[rows], dst.at[rows], send_sem.at[i], recv_sem.at[i], j)

    def far_out(i):
        return block(s_far, r_far, df_send, df_recv, direct, i, half + i)

    def near_out(i):
        return block(s_near, r_near, dn_send, dn_recv, cap, i, i)

    def over_out(i):
        return block(o_send, o_recv, do_send, do_recv, over, i, i)

    def far_back(i):
        return block(y_far, b_far, rf_send, rf_recv, direct, i, half + i)

    def near_back(i):
        return block(y_near, b_near, rn_send, rn_recv, cap, i, i)

    def over_back(i):
        return block(o_res, o_ret, ro_send, ro_recv, over, i, i)

    meta_out = remote(meta_s, meta_r, m_sem.at[0], m_sem.at[1], half)
    packet_out = remote(p_send, p_recv, p_sem.at[0], p_sem.at[1], half)
    packet_back = remote(p_pack, p_back, pb_sem.at[0], pb_sem.at[1], half)
    rounds = [remote(flag_s.at[k], flag_r.at[k], f_sem.at[k, 0], f_sem.at[k, 1], j) for k, j in enumerate((4, 2, 1))]
    rounds.append(pltpu.make_async_remote_copy(
        src_ref=flag_s.at[3], dst_ref=flag_r.at[3], send_sem=f_sem.at[3, 0], recv_sem=f_sem.at[3, 1],
        device_id=(1 - dp, my_b, my_a), device_id_type=MESH))

    barrier = pltpu.get_barrier_semaphore()

    def greet(j, carry):
        b, a = place(j)
        pl.semaphore_signal(barrier, inc=1, device_id=(dp, b, a), device_id_type=MESH)
        return carry

    lax.fori_loop(1, num_experts, lambda k, c: greet(num_experts - k, c), 0)
    pl.semaphore_signal(barrier, inc=1, device_id=(1 - dp, my_b, my_a), device_id_type=MESH)
    loads = [pltpu.make_async_copy(s, d, load_sem.at[k]) for k, (s, d) in enumerate([
        (ids_hbm, ids_ref), (order_hbm, order_ref), (tok_hbm.at[0], tok),
        (wr_hbm, wr), (keys_hbm, keys_ref), (tau_hbm, tau_ref), (b1_hbm, b1_ref), (b2_hbm, b2_ref),
        (w1_hbm.at[0], w1), (w2_hbm.at[0], w2)])]
    for c in loads[:8]:
        c.start()

    loads[0].wait()
    loads[1].wait()
    ids = ids_ref[...]
    hot, hot_f, slot, count = rank_tokens(ids, order_ref[...], perm, num_experts, cap)
    key_row = ids * LANES + slot

    e_col = lax.broadcasted_iota(I32, (num_experts, 1), 0)
    extra = jnp.where(lax.div(e_col, half) != my_half, jnp.clip(count - float(direct), 0.0, float(over)), 0.0)
    extra_b = jnp.broadcast_to(extra, (num_experts, LANES))
    below = jnp.where(lax.broadcasted_iota(I32, (num_experts, num_experts), 1) < lax.broadcasted_iota(I32, (num_experts, num_experts), 0), 1.0, 0.0)
    base_b = jnp.dot(below.astype(BF16), extra_b.astype(BF16), preferred_element_type=F32)
    total_b = base_b[num_experts - 1:, :] + extra_b[num_experts - 1:, :]
    my_flag = jnp.broadcast_to(jnp.where(total_b > float(packet), 1.0, 0.0), (8, LANES))
    diagonal = lax.broadcasted_iota(I32, (num_experts, LANES), 0) == lax.broadcasted_iota(I32, (num_experts, LANES), 1)

    def as_row(column):
        return jnp.sum(jnp.where(diagonal, column, 0.0), axis=0, keepdims=True)

    kind = lax.broadcasted_iota(I32, meta_s.shape, 0)
    meta_s[...] = jnp.where(kind == 0, as_row(base_b), jnp.where(kind == 1, as_row(extra_b), my_flag))
    base_tok = jnp.sum(hot_f * base_b[:, 0:1], axis=0, keepdims=True).astype(I32)
    is_extra = (lax.div(ids, half) != my_half) & (slot >= direct) & (slot < cap)
    q_row = jnp.where(is_extra, base_tok + slot - direct, -1)

    loads[2].wait()
    for c in loads[8:]:
        c.start()

    def gathered(mask):
        return jnp.dot(one(mask), tok[...], preferred_element_type=F32).astype(BF16)

    def two(first, second, size, axis, other):
        shape = (2 * size, other) if axis == 0 else (other, 2 * size)
        at = lax.broadcasted_iota(I32, shape, axis)
        return jnp.where(at < size, first * LANES + at, second * LANES + at - size)

    def far_keys(b, axis, other):
        return two(expert_of(half + 2 * b), expert_of(half + 2 * b + 1), direct, axis, other)

    def near_keys(b, axis, other):
        return two(expert_of(2 * b), expert_of(2 * b + 1), cap, axis, other)

    p_send[...] = gathered(lax.broadcasted_iota(I32, (packet, tok_dev), 0) == q_row)
    s_far[:2 * direct, :] = gathered(key_row == far_keys(0, 0, tok_dev))
    pl.semaphore_wait(barrier, num_experts)
    meta_out.start()
    packet_out.start()
    first = gathered(key_row == near_keys(0, 0, tok_dev))
    far_out(0).start()
    far_out(1).start()
    r_near[:cap, :] = first[:cap]
    s_near[cap:2 * cap, :] = first[cap:]

    def fill(b, c):
        s_far[span(2 * direct * b, 2 * direct), :] = gathered(key_row == far_keys(b, 0, tok_dev))
        s_near[span(2 * cap * b, 2 * cap), :] = gathered(key_row == near_keys(b, 0, tok_dev))
        return c

    lax.fori_loop(1, steps, fill, 0)
    for i in range(2, 2 * early):
        far_out(i).start()

    for c in loads[3:6]:
        c.wait()
    make_gates(tok, wr, keys_ref, tau_ref[0], hot, gate_b, [(key_b, key_row.astype(F32)), (q_b, q_row.astype(F32))])

    meta_out.wait_recv()
    packet_out.wait_recv()
    q_lane = lax.broadcasted_iota(I32, (over, packet), 1).astype(F32)
    r_sub = lax.broadcasted_iota(I32, (over, packet), 0).astype(F32)
    e_lane = lax.broadcasted_iota(I32, (1, LANES), 1)
    picks = []
    lane = lax.broadcasted_iota(I32, (1, half * over), 1)
    home = jnp.full((1, half * over), -1.0, F32)
    for j in range(half):
        e = expert_of(j)
        base, size = (jnp.sum(jnp.where(e_lane == e, meta_r[k:k + 1, :], 0.0), axis=1, keepdims=True) for k in range(2))
        picks.append(one((q_lane - r_sub) == base))
        at = (lane - j * over).astype(F32)
        home = jnp.where((at >= 0.0) & (at < size), base + at, home)
    forward = jnp.dot(jnp.concatenate(picks, axis=0), p_recv[...], preferred_element_type=F32).astype(BF16)
    o_recv[:over, :] = forward[:over]
    o_send[over:, :] = forward[over:]
    known = jnp.maximum(my_flag, meta_r[2:3, :])
    flag_s[0] = known
    unpack = one(lax.broadcasted_iota(I32, (packet, half * over), 0).astype(F32) == home)

    def start_all(make):
        def go(i, c):
            make(i).start()
            return c
        lax.fori_loop(1, half, go, 0)

    start_all(over_out)
    rounds[0].start()
    near_out(1).start()

    def dispatch(b, c):
        @pl.when(b >= early)
        def _():
            far_out(2 * b).start()
            far_out(2 * b + 1).start()

        near_out(2 * b).start()
        near_out(2 * b + 1).start()
        return c

    lax.fori_loop(1, steps, dispatch, 0)
    for c in loads[6:]:
        c.wait()

    def expert(src, dst, start, size):
        run_expert((w1, w2, b1_ref, b2_ref, hbuf), src, dst, span(start, size), size)

    def next_round(k):
        rounds[k].wait_recv()
        if k + 1 < len(rounds):
            flag_s[k + 1] = jnp.maximum(flag_s[k], flag_r[k])

    def step(b, c):
        far_out(2 * b).wait_recv()
        far_out(2 * b + 1).wait_recv()
        expert(r_far, y_far, 2 * direct * b, 2 * direct)
        far_back(2 * b).start()
        far_back(2 * b + 1).start()

        @pl.when(b > 0)
        def _():
            near_out(2 * b).wait_recv()

        near_out(2 * b + 1).wait_recv()
        expert(r_near, y_near, 2 * cap * b, 2 * cap)

        @pl.when(b > 0)
        def _():
            near_back(2 * b).start()

        near_back(2 * b + 1).start()

        @pl.when(b == 2)
        def _():
            def arrived(i, c):
                over_out(i).wait_recv()
                return c

            lax.fori_loop(1, half, arrived, 0)
            expert(o_recv, o_res, 0, half * over)
            o_ret[:over, :] = o_res[:over, :]
            start_all(over_back)

        @pl.when(b == 1)
        def _():
            next_round(0)
            rounds[1].start()

        return c

    unpack_ref[...] = unpack
    lax.fori_loop(0, steps, step, 0)
    b_near[:cap, :] = y_near[:cap, :]
    next_round(1)

    def returned(i, c):
        over_back(i).wait_recv()
        return c

    lax.fori_loop(1, half, returned, 0)
    p_pack[...] = jnp.dot(unpack_ref[...], o_ret[...], preferred_element_type=F32).astype(BF16)
    rounds[2].start()
    packet_back.start()

    def add(ref, start, keys, src, fresh=False):
        size = keys.shape[1]
        for t in range(0, tok_dev, blk):
            one_hot = one(ref[t:t + blk, :size] == keys)
            part = jnp.dot(one_hot, src[span(start, size), :], preferred_element_type=F32)
            acc[t:t + blk, :] = part if fresh else acc[t:t + blk, :] + part

    far_back(0).wait_recv()
    far_back(1).wait_recv()
    add(key_b, 0, far_keys(0, 1, 1).astype(F32), b_far, fresh=True)
    next_round(2)

    def near_sum(b, c):
        @pl.when(b > 0)
        def _():
            near_back(2 * b).wait_recv()
        near_back(2 * b + 1).wait_recv()
        add(key_b, 2 * cap * b, near_keys(b, 1, 1).astype(F32), b_near)
        return c

    lax.fori_loop(0, steps, near_sum, 0)
    rounds[3].start()

    def far_sum(b, c):
        far_back(2 * b).wait_recv()
        far_back(2 * b + 1).wait_recv()
        add(key_b, 2 * direct * b, far_keys(b, 1, 1).astype(F32), b_far)
        return c

    far_sum(1, 0)
    packet_back.wait_recv()
    add(q_b, 0, lax.broadcasted_iota(I32, (1, packet), 1).astype(F32), p_back)
    next_round(3)
    flag_s[4] = jnp.maximum(flag_s[3], flag_r[3])
    far_sum(2, 0)
    flag_out[0] = flag_s[4][0, 0].astype(I32)
    far_back(half - 2).wait_recv()
    far_back(half - 1).wait_recv()
    keys = far_keys(steps - 1, 1, 1).astype(F32)
    for t in range(0, tok_dev, blk):
        one_hot = one(key_b[t:t + blk, 0:2 * direct] == keys)
        total = acc[t:t + blk, :] + jnp.dot(one_hot, b_far[direct * (half - 2):, :], preferred_element_type=F32)
        gate = gate_b[t:t + blk, :]
        for w in range(0, width, LANES):
            out[0, t:t + blk, w:w + LANES] = (gate * total[:, w:w + LANES]).astype(BF16)

    def drain_far(i, c):
        far_out(i).wait_send()
        far_back(i).wait_send()
        return c

    def drain(i, c):
        near_out(i).wait_send()
        near_back(i).wait_send()
        over_out(i).wait_send()
        over_back(i).wait_send()
        return c

    lax.fori_loop(0, half, drain_far, 0)
    lax.fori_loop(1, half, drain, 0)
    for c in [meta_out, packet_out, packet_back] + rounds:
        c.wait_send()


def solution(mesh):
    nb, na = mesh.shape["ep_b"], mesh.shape["ep_a"]
    num_experts = nb * na
    half = num_experts // 2
    tok_spec = P(("dp",) + EXPERT_AXES)
    expert_spec = P(EXPERT_AXES)

    def device_step(tokens, expert_ids, route_order, w_route, expert_keys, value_a11, w_in, b_in, w_out, b_out):
        tok_dev, width = tokens.shape[1], tokens.shape[2]
        hidden = w_in.shape[2]
        cap = (5 * tok_dev + 4 * num_experts - 1) // (4 * num_experts)
        direct = 3 * tok_dev // (4 * num_experts)
        over = cap - direct
        packet = 21 * tok_dev // 128
        slots = num_experts * cap
        vmem = pl.BlockSpec(memory_space=pltpu.VMEM)
        hbm = pl.BlockSpec(memory_space=pl.ANY)
        dma = pltpu.SemaphoreType.DMA

        def rows(n, dtype=BF16, lanes=width):
            return pltpu.VMEM((n, lanes), dtype)

        operands = [
            pltpu.SMEM((1,), F32),
            rows(1, I32, tok_dev),
            rows(1, I32, tok_dev),
            rows(num_experts, BF16, expert_keys.shape[1]),
            rows(1, BF16, hidden),
            rows(1),
            rows(tok_dev),
            rows(width, BF16, w_route.shape[1]),
            rows(width, BF16, hidden),
            rows(hidden),
            rows(tok_dev, BF16, tok_dev),
        ]
        args = (value_a11.reshape(1), expert_ids, route_order, w_route, expert_keys, b_in, b_out, tokens, w_in, w_out)
        result = pltpu.VMEM((1, tok_dev, width), BF16)

        def full(*args):
            return pl.pallas_call(
                functools.partial(full_kernel, (nb, na, cap)),
                out_shape=result,
                in_specs=[hbm] * 10,
                out_specs=vmem,
                scratch_shapes=operands + [
                    rows(slots), rows(slots), rows(slots), rows(slots),
                    rows(2 * cap, BF16, hidden),
                    rows(tok_dev, F32, 256),
                    rows(tok_dev, F32, 128),
                    rows(tok_dev, F32),
                    rows(tok_dev, BF16, 2 * cap),
                    dma((10,)),
                ] + [dma((num_experts,))] * 4,
                compiler_params=pltpu.CompilerParams(collective_id=1, has_side_effects=True, vmem_limit_bytes=56 * 2**20),
                name="full_exchange",
            )(*args)

        far, near, extra = half * direct, half * cap, half * over
        out, flag = pl.pallas_call(
            functools.partial(tight_kernel, (nb, na, cap, direct, packet)),
            out_shape=(result, pltpu.SMEM((1,), I32)),
            in_specs=[hbm] * 10,
            out_specs=(vmem, pl.BlockSpec(memory_space=pltpu.SMEM)),
            scratch_shapes=operands + [
                rows(far), rows(near), rows(far), rows(near), rows(far), rows(near), rows(far), rows(near),
                rows(packet), rows(packet), rows(packet), rows(packet),
                rows(extra), rows(extra), rows(extra), rows(extra),
                rows(8, F32, 128), rows(8, F32, 128),
                pltpu.VMEM((5, 8, 128), F32), pltpu.VMEM((4, 8, 128), F32),
                rows(max(extra, 2 * cap), BF16, hidden),
                rows(tok_dev, F32, 256),
                rows(tok_dev, F32, 256),
                rows(tok_dev, F32, 128),
                rows(tok_dev, F32),
                rows(packet, BF16, extra),
                dma((10,)), dma((2,)), dma((2,)), dma((2,)), dma((4, 2)),
            ] + [dma((half,))] * 12,
            compiler_params=pltpu.CompilerParams(collective_id=0, has_side_effects=True, vmem_limit_bytes=61 * 2**20),
            name="tight_exchange",
        )(*args)
        return lax.cond(flag[0] > 0, lambda out, *args: full(*args), lambda out, *args: out, out, *args)

    return jax.shard_map(
        device_step,
        mesh=mesh,
        in_specs=(tok_spec, tok_spec, tok_spec, P(), P(), P(), expert_spec, expert_spec, expert_spec, expert_spec),
        out_specs=tok_spec,
        check_vma=False,
    )
```
